32 devices in a mesh: fsdp: 8 (over z, core), cols: 4 (over y, x).
Axes of the slice: x: 2, y: 2, z: 4, core: 2. Of those that a mesh axis runs over, the one named last changes fastest.
Arguments:
- weight_query: bfloat16 [5120, 5120], P('fsdp', 'cols'), may hold values from -0.078125 to 0.078125
- low_query: bfloat16 [5120, 32], P('fsdp'), may hold values from -0.078125 to 0.078125
- high_query: bfloat16 [32, 5120], P(None, 'cols'), may hold values from -1 to 1
- weight_key: bfloat16 [5120, 5120], P('fsdp', 'cols'), may hold values from -0.078125 to 0.078125
- low_key: bfloat16 [5120, 32], P('fsdp'), may hold values from -0.078125 to 0.078125
- high_key: bfloat16 [32, 5120], P(None, 'cols'), may hold values from -1 to 1
- weight_value: bfloat16 [5120, 5120], P('fsdp', 'cols'), may hold values from -0.078125 to 0.078125
- low_value: bfloat16 [5120, 32], P('fsdp'), may hold values from -0.078125 to 0.078125
- high_value: bfloat16 [32, 5120], P(None, 'cols'), may hold values from -1 to 1
- weight_mixed: bfloat16 [5120, 5120], P('cols', 'fsdp'), may hold values from -0.078125 to 0.078125
- low_mixed: bfloat16 [5120, 32], P('cols'), may hold values from -0.078125 to 0.078125
- high_mixed: bfloat16 [32, 5120], P(None, 'fsdp'), may hold values from -1 to 1
- norm_train: float32 [5120], P(('fsdp', 'cols')), may hold values from 0.25 to 1.75
- norm_step: float32 [5120], P(('fsdp', 'cols')), may hold values from -0.3 to 0.3
Outputs:
- ready_query: bfloat16 [5120, 5120], P(None, 'cols')
- ready_key: bfloat16 [5120, 5120], P(None, 'cols')
- ready_value: bfloat16 [5120, 5120], P(None, 'cols')
- ready_mixed: bfloat16 [5120, 5120], P('cols')
- serve_norm: bfloat16 [5120], replicated
The draws below stay inside these ranges and needn't reach their ends.
All inputs are finite; a program needn't handle non-finite values.
Results may differ from the reference program's by a relative error of at most 0.001.
Values may be sent and summed in bfloat16 or wider, within the bound.
A program may use at most 192 MiB of HBM per device.

```python
import jax
import jax.numpy as jnp

D_MODEL = 5120
Q_DIM = 5120
KV_DIM = 5120
RANK = 32


def block_levels(stream_key, extent, pieces, smallest, high):
    level, own = 1.0, jax.random.fold_in(stream_key, 6)
    for dim, shards_of in pieces:
        steps = jnp.exp(jax.random.uniform(jax.random.fold_in(own, dim), (shards_of,), jnp.float32, smallest / len(pieces), high / len(pieces)))
        level = level * jnp.repeat(steps, extent[dim] // shards_of).reshape([-1 if axis == dim else 1 for axis in range(len(extent))])
    return level


def gaussian(stream_key, extent, deviation, limit, split=(), dtype=jnp.bfloat16):
    values = deviation * jax.random.normal(stream_key, extent, jnp.float32)
    if split:
        values = values * block_levels(stream_key, extent, split, -0.22, 0.18)
    return jnp.clip(values, -limit, limit).astype(dtype)


def setup_inputs(seed: int = 0) -> dict:
    arg_keys = jax.random.split(jax.random.key(seed), 15)
    weight_query = gaussian(arg_keys[0], (D_MODEL, Q_DIM), D_MODEL ** -0.5, 0.078125, ((0, 8), (1, 4)))
    low_query = gaussian(arg_keys[1], (D_MODEL, RANK), D_MODEL ** -0.5, 0.078125, ((0, 8),))
    high_query = gaussian(arg_keys[2], (RANK, Q_DIM), RANK ** -0.5, 1.0, ((1, 4),))
    weight_key = gaussian(arg_keys[3], (D_MODEL, KV_DIM), D_MODEL ** -0.5, 0.078125, ((0, 8), (1, 4)))
    low_key = gaussian(arg_keys[4], (D_MODEL, RANK), D_MODEL ** -0.5, 0.078125, ((0, 8),))
    high_key = gaussian(arg_keys[5], (RANK, KV_DIM), RANK ** -0.5, 1.0, ((1, 4),))
    weight_value = gaussian(arg_keys[6], (D_MODEL, KV_DIM), D_MODEL ** -0.5, 0.078125, ((0, 8), (1, 4)))
    low_value = gaussian(arg_keys[7], (D_MODEL, RANK), D_MODEL ** -0.5, 0.078125, ((0, 8),))
    high_value = gaussian(arg_keys[8], (RANK, KV_DIM), RANK ** -0.5, 1.0, ((1, 4),))
    weight_mixed = gaussian(arg_keys[9], (Q_DIM, D_MODEL), Q_DIM ** -0.5, 0.078125, ((0, 4), (1, 8)))
    low_mixed = gaussian(arg_keys[10], (Q_DIM, RANK), Q_DIM ** -0.5, 0.078125, ((0, 4),))
    high_mixed = gaussian(arg_keys[11], (RANK, D_MODEL), RANK ** -0.5, 1.0, ((1, 8),))
    norm_train = jnp.clip(1.0 + 0.15 * jax.random.normal(arg_keys[12], (D_MODEL,), jnp.float32), 0.25, 1.75)
    norm_step = jnp.clip(jax.random.uniform(arg_keys[13], (D_MODEL,), jnp.float32, -0.3, 0.3) * block_levels(arg_keys[13], (D_MODEL,), ((0, 32),), -0.4, 0.0), -0.3, 0.3)
    return dict(weight_query=weight_query, low_query=low_query, high_query=high_query, weight_key=weight_key, low_key=low_key, high_key=high_key, weight_value=weight_value, low_value=low_value, high_value=high_value, weight_mixed=weight_mixed, low_mixed=low_mixed, high_mixed=high_mixed, norm_train=norm_train, norm_step=norm_step)


mix_rate = 2.0


def reference(weight_query, low_query, high_query, weight_key, low_key, high_key, weight_value, low_value, high_value, weight_mixed, low_mixed, high_mixed, norm_train, norm_step):
    latest_query = weight_query.astype(jnp.float32) + mix_rate * jnp.dot(low_query, high_query, preferred_element_type=jnp.float32)
    latest_key = weight_key.astype(jnp.float32) + mix_rate * jnp.dot(low_key, high_key, preferred_element_type=jnp.float32)
    latest_value = weight_value.astype(jnp.float32) + mix_rate * jnp.dot(low_value, high_value, preferred_element_type=jnp.float32)
    latest_mixed = weight_mixed.astype(jnp.float32) + mix_rate * jnp.dot(low_mixed, high_mixed, preferred_element_type=jnp.float32)
    ready_query = latest_query.astype(jnp.bfloat16)
    ready_key = latest_key.astype(jnp.bfloat16)
    ready_value = latest_value.astype(jnp.bfloat16)
    ready_mixed = latest_mixed.astype(jnp.bfloat16)
    serve_norm = (norm_train + norm_step).astype(jnp.bfloat16)
    return ready_query, ready_key, ready_value, ready_mixed, serve_norm
```

```python
import functools

import jax
import jax.numpy as jnp
from jax import lax
from jax.experimental import pallas as pl
from jax.experimental.pallas import tpu as pltpu
from jax.sharding import PartitionSpec as P

mix_rate = 2.0
MESH = pl.DeviceIdType.MESH
ROW_TILE = 128
BY_ROWS = (True, True, False, True)
LAST = len(BY_ROWS) - 1


def block_of(ref, by_rows, index, extent):
    if len(ref.shape) == 3:
        return ref.at[index]
    if by_rows:
        return ref.at[pl.ds(pl.multiple_of(index * extent, extent), extent), :]
    return ref.at[:, pl.ds(pl.multiple_of(index * extent, extent), extent)]


def gather_kernel(spots, has_tail, *refs):
    weights, lows, highs = refs[0:4], refs[4:8], refs[8:12]
    outs = refs[12:16]
    raw, ready = refs[16:20], refs[20:24]
    in_sem, own_sem, send_r, recv_r, send_l, recv_l, send_d, recv_d = refs[24:]
    me = lax.axis_index("fsdp")
    spot, core = lax.div(me, 2), lax.rem(me, 2)
    last = spots - 1
    number = len(BY_ROWS)

    loads = [pltpu.make_async_copy(weights[w], raw[w], in_sem.at[w]) for w in range(number)]
    for load in loads:
        load.start()

    barrier = pltpu.get_barrier_semaphore()

    def greet(target):
        pl.semaphore_signal(barrier, inc=1, device_id={"fsdp": target}, device_id_type=MESH)

    greet(2 * spot + 1 - core)

    @pl.when(spot > 0)
    def _():
        greet(me - 2)

    @pl.when(spot < last)
    def _():
        greet(me + 2)

    peers = 1 + (spot > 0).astype(jnp.int32) + (spot < last).astype(jnp.int32)
    pl.semaphore_wait(barrier, peers)

    def block(w, origin, side):
        extent = weights[w].shape[0 if BY_ROWS[w] else 1]
        return block_of(outs[w], BY_ROWS[w], 2 * origin + side, extent)

    def remote(w, origin, side, target, send, recv):
        piece = block(w, origin, side)
        return pltpu.make_async_remote_copy(
            src_ref=piece,
            dst_ref=piece,
            send_sem=send,
            recv_sem=recv,
            device_id={"fsdp": target},
            device_id_type=MESH,
        )

    def rightward(w, step, origin):
        return remote(w, origin, core, me + 2, send_r.at[w, step], recv_r.at[w, step])

    def leftward(w, step, origin):
        return remote(w, origin, core, me - 2, send_l.at[w, step], recv_l.at[w, step])

    def across(w, slot, origin, side):
        return remote(w, origin, side, 2 * spot + 1 - core, send_d.at[w, slot], recv_d.at[w, slot])

    def travels(w, step):
        return step <= last and not (has_tail and w == LAST and step == last)

    for w in range(number):
        loads[w].wait()
        rows = weights[w].shape[0]
        height = rows if rows % ROW_TILE else ROW_TILE

        def merge(tile, carry, w=w, height=height):
            start = pl.multiple_of(tile * height, height) if height < weights[w].shape[0] else 0
            product = lax.dot_general(
                lows[w][:, pl.ds(start, height)],
                highs[w][...],
                (((0,), (0,)), ((), ())),
                preferred_element_type=jnp.float32,
            )
            base = raw[w][pl.ds(start, height), :].astype(jnp.float32)
            ready[w][pl.ds(start, height), :] = (base + mix_rate * product).astype(jnp.bfloat16)
            return carry

        lax.fori_loop(0, rows // height, merge, 0)
        keep = pltpu.make_async_copy(ready[w], block(w, spot, core), own_sem.at[w])
        keep.start()
        keep.wait()
        if travels(w, 1):

            @pl.when(spot < last)
            def _():
                rightward(w, 1, spot).start()

            @pl.when(spot > 0)
            def _():
                leftward(w, 1, spot).start()

        across(w, 0, spot, core).start()

    for step in range(1, spots):
        for w in range(number):
            if not travels(w, step):
                continue

            @pl.when(spot - step >= 0)
            def _():
                rightward(w, step, spot - step).wait_recv()
                if travels(w, step + 1):

                    @pl.when(spot < last)
                    def _():
                        rightward(w, step + 1, spot - step).start()

                across(w, step, spot - step, core).start()

            @pl.when(spot + step <= last)
            def _():
                leftward(w, step, spot + step).wait_recv()
                if travels(w, step + 1):

                    @pl.when(spot > 0)
                    def _():
                        leftward(w, step + 1, spot + step).start()

                across(w, last + step, spot + step, core).start()

    for w in range(number):
        across(w, 0, spot, core).wait_send()
        across(w, 0, spot, 1 - core).wait_recv()
        for step in range(1, spots):
            if not travels(w, step):
                continue

            @pl.when((spot < last) & (spot - step + 1 >= 0))
            def _():
                rightward(w, step, spot - step + 1).wait_send()

            @pl.when((spot > 0) & (spot + step - 1 <= last))
            def _():
                leftward(w, step, spot + step - 1).wait_send()

            @pl.when(spot - step >= 0)
            def _():
                across(w, step, spot - step, core).wait_send()
                across(w, step, spot - step, 1 - core).wait_recv()

            @pl.when(spot + step <= last)
            def _():
                across(w, last + step, spot + step, core).wait_send()
                across(w, last + step, spot + step, 1 - core).wait_recv()


def copy_kernel(*refs):
    number = len(refs) // 2
    for w in range(number):
        refs[number + w][...] = refs[w][...]


def patch_kernel(spots, got_ref, other_ref, base_ref, out_ref, got, other, sem):
    me = lax.axis_index("fsdp")
    spot, core = lax.div(me, 2), lax.rem(me, 2)
    extent = got_ref.shape[0]

    @pl.when((spot == 0) | (spot == spots - 1))
    def _():
        origin = spots - 1 - spot
        loads = [
            pltpu.make_async_copy(got_ref, got, sem.at[0]),
            pltpu.make_async_copy(other_ref, other, sem.at[1]),
        ]
        stores = [
            pltpu.make_async_copy(
                got, block_of(out_ref, True, 2 * origin + core, extent), sem.at[2]
            ),
            pltpu.make_async_copy(
                other, block_of(out_ref, True, 2 * origin + 1 - core, extent), sem.at[3]
            ),
        ]
        for load in loads:
            load.start()
        for load, store in zip(loads, stores):
            load.wait()
            store.start()
        for store in stores:
            store.wait()


def per_device(
    fsdp,
    weight_query,
    low_query,
    high_query,
    weight_key,
    low_key,
    high_key,
    weight_value,
    low_value,
    high_value,
    weight_mixed,
    low_mixed,
    high_mixed,
    norm_train,
    norm_step,
):
    spots = fsdp // 2
    has_tail = spots >= 4
    weights = (weight_query, weight_key, weight_mixed, weight_value)
    lows = (low_query.T, low_key.T, low_mixed.T, low_value.T)
    highs = (high_query, high_key, high_mixed, high_value)
    number = len(weights)
    whole = tuple(
        jax.ShapeDtypeStruct(
            (x.shape[0] * fsdp, x.shape[1]) if by_rows else (x.shape[0], x.shape[1] * fsdp),
            jnp.bfloat16,
        )
        for x, by_rows in zip(weights, BY_ROWS)
    )
    stacked = tuple(not by_rows and x.shape[1] % 128 != 0 for x, by_rows in zip(weights, BY_ROWS))
    landing = tuple(
        jax.ShapeDtypeStruct((fsdp, *x.shape), jnp.bfloat16) if apart else full
        for x, full, apart in zip(weights, whole, stacked)
    )
    anywhere = pl.BlockSpec(memory_space=pl.ANY)
    inside = pl.BlockSpec(memory_space=pltpu.VMEM)
    dma = pltpu.SemaphoreType.DMA
    gathered = pl.pallas_call(
        functools.partial(gather_kernel, spots, has_tail),
        out_shape=landing,
        in_specs=[anywhere] * number + [inside] * (2 * number),
        out_specs=[anywhere] * number,
        scratch_shapes=[pltpu.VMEM(x.shape, jnp.bfloat16) for x in weights] * 2
        + [dma((number,))] * 2
        + [dma((number, spots))] * 4
        + [dma((number, 2 * spots - 1))] * 2,
        compiler_params=pltpu.CompilerParams(
            collective_id=0, has_side_effects=True, vmem_limit_bytes=60 * 2**20
        ),
        name="gather",
    )(*weights, *lows, *highs)

    me = lax.axis_index("fsdp")
    spot, core = me // 2, me % 2
    extent = weight_value.shape[0]
    if has_tail:
        origin = jnp.where(spot == 1, spots - 1, 0)
        edge = lax.dynamic_slice_in_dim(gathered[LAST], (2 * origin + core) * extent, extent, 0)
        ends = [(2 * (spots - 2) + side, 2 * (spots - 1) + side) for side in range(2)]
        ends += [(2 + side, side) for side in range(2)]
        got = lax.ppermute(edge, "fsdp", ends)
        swap = [(i, i ^ 1) for i in (0, 1, fsdp - 2, fsdp - 1)]

    settled = [w for w in range(number) if not stacked[w]]
    specs = [
        pl.BlockSpec(weights[w].shape, (lambda i: (i, 0)) if BY_ROWS[w] else (lambda i: (0, i)))
        for w in settled
    ]
    moved = 2 * sum(2 * x.shape[0] * x.shape[1] for x in whole)
    ready = pl.pallas_call(
        copy_kernel,
        grid=(fsdp,),
        out_shape=[whole[w] for w in settled],
        in_specs=specs,
        out_specs=specs,
        compiler_params=pltpu.CompilerParams(vmem_limit_bytes=48 * 2**20),
        cost_estimate=pl.CostEstimate(flops=0, bytes_accessed=moved, transcendentals=0),
        name="settle",
    )(*[gathered[w] for w in settled])
    finished = dict(zip(settled, ready))
    for w in range(number):
        if stacked[w]:
            finished[w] = gathered[w].transpose(1, 0, 2).reshape(whole[w].shape)
    ready_query, ready_key, ready_mixed, ready_value = (finished[w] for w in range(number))
    if has_tail:
        got, ready_value = lax.optimization_barrier((got, ready_value))
        other = lax.ppermute(got, "fsdp", swap)
        ready_value = pl.pallas_call(
            functools.partial(patch_kernel, spots),
            out_shape=whole[LAST],
            in_specs=[anywhere] * 3,
            out_specs=anywhere,
            scratch_shapes=[pltpu.VMEM(weight_value.shape, jnp.bfloat16)] * 2 + [dma((4,))],
            input_output_aliases={2: 0},
            compiler_params=pltpu.CompilerParams(vmem_limit_bytes=16 * 2**20),
            name="patch",
        )(got, other, ready_value)

    serve_norm = lax.all_gather(
        (norm_train + norm_step).astype(jnp.bfloat16), ("fsdp", "cols"), axis=0, tiled=True
    )
    return (ready_query, ready_key, ready_value, ready_mixed, serve_norm)


def solution(mesh):
    in_specs = (
        P("fsdp", "cols"),
        P("fsdp", None),
        P(None, "cols"),
        P("fsdp", "cols"),
        P("fsdp", None),
        P(None, "cols"),
        P("fsdp", "cols"),
        P("fsdp", None),
        P(None, "cols"),
        P("cols", "fsdp"),
        P("cols", None),
        P(None, "fsdp"),
        P(("fsdp", "cols")),
        P(("fsdp", "cols")),
    )
    out_specs = (P(None, "cols"), P(None, "cols"), P(None, "cols"), P("cols", None), P())
    return jax.shard_map(
        functools.partial(per_device, mesh.shape["fsdp"]),
        mesh=mesh,
        in_specs=in_specs,
        out_specs=out_specs,
        check_vma=False,
    )
```
